32 devices in a mesh: grp: 2 (over y), kvp: 4 (over x, core), tp: 4 (over z).
Axes of the slice: x: 2, y: 2, z: 4, core: 2. Of those that a mesh axis runs over, the one named last changes fastest.
Arguments:
- hidden_in: bfloat16 [16, 7168], P('grp'), parts along dimension 0, may hold values from -3 to 3
- queries_nope: bfloat16 [16, 128, 128], P('grp', ('kvp', 'tp')), parts along dimension 0, may hold values from -6 to 6
- queries_rope: bfloat16 [16, 128, 64], P('grp', ('kvp', 'tp')), parts along dimension 0, may hold values from -26 to 26
- cache: bfloat16 [16, 1536, 576], P('grp', 'kvp'), parts along dimension 0, may hold values from -20 to 20
- lengths: int32 [16], P('grp'), parts along dimension 0, may hold values from 128 to 1536, as said below
- w_uk: bfloat16 [128, 128, 512], P(('kvp', 'tp')), may hold values from -0.5 to 0.5
- w_uv: bfloat16 [128, 512, 128], P(('kvp', 'tp')), may hold values from -0.25 to 0.25
- w_out: bfloat16 [16384, 7168], P(('kvp', 'tp')), may hold values from -0.0625 to 0.0625
- norm_gain: float32 [7168], replicated, may hold values from 0.25 to 1.75
- w_gate: bfloat16 [7168, 18432], P(None, ('kvp', 'tp')), may hold values from -0.0625 to 0.0625
- w_up: bfloat16 [7168, 18432], P(None, ('kvp', 'tp')), may hold values from -0.0625 to 0.0625
- w_down: bfloat16 [18432, 7168], P(('kvp', 'tp')), may hold values from -0.0625 to 0.0625
Outputs:
- layer_out: bfloat16 [16, 7168], P('grp', ('kvp', 'tp')), parts along dimension 0
The draws below stay inside these ranges and needn't reach their ends.
There are 2 independent parts, one for each index of `grp`. The reference program is written for one: setup_inputs(seed, part) draws one part's arguments, and reference() takes and returns one part's arrays. A program takes and returns all parts, laid end to end along the dimension named above; an argument that names none is the same for every part. Nothing has to cross between parts.
Inputs may be any that keep to these rules, and one draw needn't show every extreme that they name: `lengths`: every length is a multiple of 128; in every draw some request has the full 1536.
All inputs are finite; a program needn't handle non-finite values.
Results may differ from the reference program's by a relative error of at most 0.04.
Values may be sent and summed in bfloat16 or wider, within the bound.
A program may use at most 128 MiB of HBM per device.

```python
import jax
import jax.numpy as jnp
from jax import lax

D = 7168
FF = 18432
H = 128
LAT = 512
ROPE = 64
HEAD_DIM = 128
BATCH = 8
BLOCK = 128
CTX_DEV = 384
CTX = 1536
N_KVP = 4


def draw_lengths(key, part):
    count_blocks = CTX // BLOCK
    counts = jax.random.randint(key, (BATCH,), 1, count_blocks + 1)
    full_row = jax.random.randint(jax.random.fold_in(key, 3), (), 0, BATCH)
    counts = jnp.where(jnp.arange(BATCH) == full_row, count_blocks, counts)
    return (counts * BLOCK).astype(jnp.int32)


def draw_cache(key, part):
    values = jnp.clip(jax.random.normal(jax.random.fold_in(key, 11), (BATCH, CTX, LAT + ROPE), jnp.float32), -6.0, 6.0)
    return values.astype(jnp.bfloat16)


def draw_queries_rope(key, part):
    values = jnp.clip(jax.random.normal(jax.random.fold_in(key, 21), (BATCH, H, ROPE), jnp.float32), -6.0, 6.0)
    return values.astype(jnp.bfloat16)


def strengthened(drawn, key, source, target, shards_of, factor):
    def block_of(position):
        return (jnp.arange(drawn.shape[position]) // (drawn.shape[position] // shards_of)).reshape((-1,) + (1,) * (drawn.ndim - 1 - position))

    first = jax.random.permutation(key, shards_of)[block_of(target)]
    far = (block_of(target) + shards_of // 2) % shards_of
    return jnp.where((block_of(source) == first) | (block_of(source) == far), factor * drawn, drawn)


def block_scale(own_key, shape, pieces, smallest, largest):
    level = 1.0
    for position, shards_of in pieces:
        heights = jax.random.uniform(jax.random.fold_in(jax.random.fold_in(own_key, 6), position), (shards_of,), jnp.float32, smallest / len(pieces), largest / len(pieces))
        level = level * jnp.repeat(jnp.exp(heights), shape[position] // shards_of).reshape((-1,) + (1,) * (len(shape) - 1 - position))
    return level


def centred(own_key, extent, scale, most, shards=(), kind=jnp.bfloat16):
    result = jax.random.normal(own_key, extent, jnp.float32) * scale
    if len(shards) > 0:
        result = block_scale(own_key, extent, shards, -0.22, 0.18) * result
    return jnp.clip(result, min=-most, max=most).astype(kind)


def heavy_noise(own_key, extent, deviation, bound, cuts, heavy, kind=jnp.bfloat16):
    entries = deviation * jax.random.normal(own_key, extent, jnp.float32)
    if cuts:
        entries = entries * block_scale(own_key, extent, cuts, -0.22, 0.18)
    return jnp.clip(strengthened(entries, jax.random.fold_in(own_key, 3), *heavy), -bound, bound).astype(kind)


def setup_inputs(seed: int = 0, part: int = 0) -> dict:
    key_of = jax.random.split(jax.random.key(seed), 13)
    own_keys = jax.random.split(jax.random.fold_in(key_of[12], part), 13)
    hidden_in = centred(own_keys[0], (BATCH, D), 0.5, 3.0)
    queries_nope = centred(own_keys[1], (BATCH, H, HEAD_DIM), 1.0, 6.0, ((1, 16),))
    queries_rope = draw_queries_rope(jax.random.fold_in(jax.random.fold_in(key_of[12], part), 71), part)
    cache = draw_cache(jax.random.fold_in(jax.random.fold_in(key_of[12], part), 71), part)
    lengths = draw_lengths(jax.random.fold_in(jax.random.fold_in(key_of[12], part), 71), part)
    w_uk = centred(key_of[5], (H, HEAD_DIM, LAT), HEAD_DIM ** -0.5, 0.5, ((0, 16),))
    w_uv = centred(key_of[6], (H, LAT, HEAD_DIM), LAT ** -0.5, 0.25, ((0, 16),))
    w_out = heavy_noise(key_of[7], (H * HEAD_DIM, D), (H * HEAD_DIM) ** -0.5, 0.0625, ((0, 16),), (0, 1, 16, 2.0))
    norm_gain = jnp.clip(1.0 + 0.15 * jax.random.normal(key_of[8], (D,), jnp.float32), 0.25, 1.75)
    w_gate = centred(key_of[9], (D, FF), D ** -0.5, 0.0625, ((1, 16),))
    w_up = centred(key_of[10], (D, FF), D ** -0.5, 0.0625, ((1, 16),))
    w_down = heavy_noise(key_of[11], (FF, D), FF ** -0.5, 0.0625, ((0, 16),), (0, 1, 16, 2.0))
    return {"hidden_in": hidden_in, "queries_nope": queries_nope, "queries_rope": queries_rope, "cache": cache, "lengths": lengths, "w_uk": w_uk, "w_uv": w_uv, "w_out": w_out, "norm_gain": norm_gain, "w_gate": w_gate, "w_up": w_up, "w_down": w_down}


def reference(hidden_in, queries_nope, queries_rope, cache, lengths, w_uk, w_uv, w_out, norm_gain, w_gate, w_up, w_down):
    score_scale = float(HEAD_DIM + ROPE) ** (-0.5)
    q_lat = jnp.einsum('bhd,hdl->bhl', queries_nope.astype(jnp.float32), w_uk.astype(jnp.float32)).astype(jnp.bfloat16)
    q_full = jnp.concatenate([q_lat, queries_rope], axis=2).astype(jnp.float32)
    cache_wide = cache.astype(jnp.float32)
    scores = jnp.einsum('bhc,btc->bht', q_full, cache_wide) * score_scale
    visible = jnp.arange(CTX, dtype=jnp.int32)[None, :] < lengths[:, None]
    visible = jnp.broadcast_to(visible[:, None, :], scores.shape).reshape(BATCH, H, N_KVP, CTX_DEV)
    blocks = scores.reshape(BATCH, H, N_KVP, CTX_DEV)
    masked = jnp.where(visible, blocks, jnp.float32(-1e+30))
    block_max = lax.optimization_barrier(jnp.max(masked, axis=3))
    exponent = jnp.where(visible, jnp.exp(masked - block_max[..., None]), jnp.float32(0.0))
    block_sum = lax.optimization_barrier(jnp.sum(exponent, axis=3))
    guarded = jnp.maximum(block_sum, 1.0)
    log_total = block_max + jnp.log(guarded)
    weights = (exponent / guarded[..., None]).astype(jnp.bfloat16)
    cache_blocks = cache_wide.reshape(BATCH, N_KVP, CTX_DEV, LAT + ROPE)
    partial_value = jnp.einsum('bhkt,bktc->bhkc', weights.astype(jnp.float32), cache_blocks)[..., :LAT]
    highest = lax.optimization_barrier(jnp.max(log_total, axis=2))
    overall = highest + jnp.log(lax.optimization_barrier(jnp.sum(jnp.exp(log_total - highest[..., None]), axis=2)))
    o_lat = lax.optimization_barrier(jnp.sum(jnp.exp(log_total - overall[..., None])[..., None] * partial_value, axis=2)).astype(jnp.bfloat16)
    head_out = jnp.einsum('bhl,hle->bhe', o_lat.astype(jnp.float32), w_uv.astype(jnp.float32)).astype(jnp.bfloat16)
    attention = jnp.dot(head_out.reshape(BATCH, H * HEAD_DIM), w_out, preferred_element_type=jnp.float32)
    residual = hidden_in.astype(jnp.float32) + attention
    mean_square = lax.optimization_barrier(jnp.mean(residual * residual, axis=1))
    normed = (residual * lax.rsqrt(mean_square + 1e-06)[:, None] * norm_gain.astype(jnp.float32)[None, :]).astype(jnp.bfloat16)
    gate_proj = jnp.dot(normed, w_gate, preferred_element_type=jnp.float32)
    up_proj = jnp.dot(normed, w_up, preferred_element_type=jnp.float32)
    act = (jax.nn.silu(gate_proj) * up_proj).astype(jnp.bfloat16)
    ffn_out = jnp.dot(act, w_down, preferred_element_type=jnp.float32)
    return (residual + ffn_out).astype(jnp.bfloat16)
```

```python
import functools

import jax
import jax.numpy as jnp
from jax import lax
from jax.experimental import pallas as pl
from jax.experimental.pallas import tpu as pltpu
from jax.sharding import PartitionSpec as P


def project(o_lat, w_uv, w_out):
    head_out = jnp.einsum("bhl,hle->bhe", o_lat, w_uv, preferred_element_type=jnp.float32).astype(
        jnp.bfloat16
    )
    return jnp.dot(
        head_out.reshape(head_out.shape[0], -1), w_out, preferred_element_type=jnp.float32
    )


def plain_device(
    hidden_in,
    queries_nope,
    queries_rope,
    cache,
    lengths,
    w_uk,
    w_uv,
    w_out,
    norm_gain,
    w_gate,
    w_up,
    w_down,
):
    batch, heads_dev, head_dim = queries_nope.shape
    latent = w_uk.shape[2]
    ctx_dev = cache.shape[1]
    groups = lax.axis_size("kvp")
    score_scale = float(head_dim + queries_rope.shape[2]) ** (-0.5)
    q_lat = jnp.einsum(
        "bhd,hdl->bhl", queries_nope, w_uk, preferred_element_type=jnp.float32
    ).astype(jnp.bfloat16)
    q_lat_all, rope_all = (
        lax.all_gather(q_lat, "kvp", axis=1, tiled=True),
        lax.all_gather(queries_rope, "kvp", axis=1, tiled=True),
    )
    q_full = jnp.concatenate([q_lat_all, rope_all], axis=2)
    scores = (
        jnp.einsum("bhc,btc->bht", q_full, cache, preferred_element_type=jnp.float32) * score_scale
    )
    offset = lax.axis_index("kvp") * ctx_dev
    visible = ((offset + jnp.arange(ctx_dev, dtype=jnp.int32))[None, :] < lengths[:, None])[
        :, None, :
    ]
    masked = jnp.where(visible, scores, jnp.float32(-1e30))
    block_max = jnp.max(masked, axis=2)
    exponent = jnp.where(visible, jnp.exp(masked - block_max[..., None]), jnp.float32(0.0))
    guarded = jnp.maximum(jnp.sum(exponent, axis=2), 1.0)
    log_total = block_max + jnp.log(guarded)
    weights = (exponent / guarded[..., None]).astype(jnp.bfloat16)
    partial_value = jnp.einsum("bht,btc->bhc", weights, cache, preferred_element_type=jnp.float32)[
        ..., :latent
    ]
    blocks = partial_value.reshape(batch, groups, heads_dev, latent)
    block_logs = log_total.reshape(batch, groups, heads_dev)
    part_blocks = lax.all_to_all(
        blocks.astype(jnp.bfloat16), "kvp", split_axis=1, concat_axis=1, tiled=True
    ).astype(blocks.dtype)
    part_logs = lax.all_to_all(
        block_logs.astype(jnp.bfloat16), "kvp", split_axis=1, concat_axis=1, tiled=True
    ).astype(block_logs.dtype)
    highest = jnp.max(part_logs, axis=1)
    overall = highest + jnp.log(jnp.sum(jnp.exp(part_logs - highest[:, None, :]), axis=1))
    scaled = jnp.exp(part_logs - overall[:, None, :])[..., None] * part_blocks
    o_lat = jnp.sum(scaled, axis=1).astype(jnp.bfloat16)
    attention = project(o_lat, w_uv, w_out)
    model_width = norm_gain.shape[0]
    share_width = model_width // lax.axis_size(("kvp", "tp"))
    share_start = lax.axis_index(("kvp", "tp")) * share_width
    attn_whole = lax.psum(attention, ("kvp", "tp"))
    residual = hidden_in.astype(jnp.float32) + attn_whole
    mean_square = jnp.mean(residual * residual, axis=1)
    normed = (residual * lax.rsqrt(mean_square + 1e-06)[:, None] * norm_gain[None, :]).astype(
        jnp.bfloat16
    )
    residual_share = lax.dynamic_slice_in_dim(residual, share_start, share_width, 1)
    gate_proj = jnp.dot(normed, w_gate, preferred_element_type=jnp.float32)
    up_proj = jnp.dot(normed, w_up, preferred_element_type=jnp.float32)
    act = (jax.nn.silu(gate_proj) * up_proj).astype(jnp.bfloat16)
    ffn_terms = jnp.dot(act, w_down, preferred_element_type=jnp.float32)
    ffn_share = lax.psum_scatter(ffn_terms, ("kvp", "tp"), scatter_dimension=1, tiled=True)
    return (residual_share + ffn_share).astype(jnp.bfloat16)


MESH = pl.DeviceIdType.MESH
F32 = jnp.float32
BF16 = jnp.bfloat16
VMEM_BYTES = 67043328


def layer_kernel(
    groups, tps, share, chunk, out_rows,
    hidden_ref, nope_ref, rope_ref, len_ref, gain_ref,
    cache_hbm, uk_hbm, uv_hbm, wo_hbm, wg_hbm, wu_hbm, wd_hbm,
    out_ref,
    cache_v, uk_v, uv_v, big_v, wg_v, wu_v,
    nope_s, qlat_s, q_send, q_all, score_s, part_send, part_all, log_send, log_all,
    olat_s, head_s, hid_s, rs_send, rs_all, ag_send, ag_all, wide_s, norm_s, fs_send, fs_all,
    uk_sem, cache_sem, uv_sem, wo_sem, wg_sem, wu_sem, wd_sem,
    q_ss, q_rs, part_ss, part_rs, log_ss, log_rs, rs_ss, rs_rs, ag_ss, ag_rs, fs_ss, fs_rs,
):
    count = groups * tps
    kvp = lax.axis_index("kvp")
    tp = lax.axis_index("tp")
    me = kvp * tps + tp
    batch, heads, head_dim = nope_ref.shape
    latent = uk_v.shape[2]
    rope = rope_ref.shape[2]
    ctx = cache_v.shape[1]
    width = hidden_ref.shape[1]
    chunks = width // chunk
    per_chunk = chunk // share

    def peer(index):
        return {"kvp": index // tps, "tp": index % tps}

    def load_uk():
        return pltpu.make_async_copy(uk_hbm, uk_v, uk_sem)

    def load_cache():
        return pltpu.make_async_copy(cache_hbm, cache_v, cache_sem)

    def load_uv():
        return pltpu.make_async_copy(uv_hbm, uv_v, uv_sem)

    def cols(j):
        return pl.ds(pl.multiple_of(j * chunk, 128), chunk)

    def load_wo(j):
        return pltpu.make_async_copy(
            wo_hbm.at[:, cols(j)], big_v.at[j, pl.ds(0, out_rows)], wo_sem.at[j]
        )

    def load_wd(j):
        return pltpu.make_async_copy(wd_hbm.at[:, cols(j)], big_v.at[j], wd_sem.at[j])

    def load_wg(j):
        return pltpu.make_async_copy(wg_hbm.at[cols(j)], wg_v.at[cols(j)], wg_sem.at[j])

    def load_wu(j):
        return pltpu.make_async_copy(wu_hbm.at[cols(j)], wu_v.at[cols(j)], wu_sem.at[j])

    load_uk().start()
    load_cache().start()

    barrier = pltpu.get_barrier_semaphore()

    @pl.loop(1, count)
    def _(d):
        pl.semaphore_signal(
            barrier, inc=1, device_id=peer(lax.rem(me + d, count)), device_id_type=MESH
        )

    nope_s[...] = nope_ref[...].astype(F32)
    for s in range(count):
        hid_s[s] = hidden_ref[:, s * share : (s + 1) * share].astype(F32)
    load_uk().wait()
    load_uv().start()

    @pl.loop(0, chunks)
    def _(j):
        load_wo(j).start()

    for i in range(heads):
        qlat_s[:, i, :] = jnp.dot(
            nope_s[:, i, :].astype(BF16), uk_v[i], preferred_element_type=F32
        )
    q_send[:, :, :latent] = qlat_s[...].astype(BF16)
    q_send[:, :, latent:] = rope_ref[...]
    pl.semaphore_wait(barrier, count - 1)

    def exchange(d, source, target, ss, rs, ahead):
        other = lax.rem(kvp + d, groups) if ahead else lax.rem(kvp + groups - d, groups)
        return pltpu.make_async_remote_copy(
            src_ref=source.at[other] if source is not q_send else source,
            dst_ref=target.at[kvp if ahead else other],
            send_sem=ss.at[d],
            recv_sem=rs.at[kvp if ahead else other],
            device_id={"kvp": other, "tp": tp},
            device_id_type=MESH,
        )

    for d in range(1, groups):
        exchange(d, q_send, q_all, q_ss, q_rs, True).start()

    @pl.loop(0, chunks)
    def _(j):
        load_wg(j).start()
        load_wu(j).start()

    q_all[kvp] = q_send[...]
    load_cache().wait()
    for d in range(1, groups):
        exchange(d, q_send, q_all, q_ss, q_rs, False).wait_recv()

    scale = float(head_dim + rope) ** (-0.5)
    rows = groups * heads
    for b in range(batch):
        q = q_all[:, b].astype(F32).reshape(rows, latent + rope)
        contract = (((1,), (1,)), ((), ()))
        score_s[b] = (
            lax.dot_general(
                q[:, :latent].astype(BF16), cache_v[b, :, :latent], contract,
                preferred_element_type=F32,
            )
            + lax.dot_general(
                q[:, latent:].astype(BF16), cache_v[b, :, latent:], contract,
                preferred_element_type=F32,
            )
        ) * scale
    position = kvp * ctx + lax.broadcasted_iota(jnp.int32, (rows, ctx), 1)
    for b in range(batch):
        visible = position < len_ref[b]
        masked = jnp.where(visible, score_s[b], F32(-1e30))
        top = jnp.max(masked, axis=1, keepdims=True)
        exps = jnp.where(visible, jnp.exp(masked - top), F32(0.0))
        guarded = jnp.maximum(jnp.sum(exps, axis=1, keepdims=True), 1.0)
        log_total = jnp.broadcast_to(top + jnp.log(guarded), (rows, 128))
        weights = (exps / guarded).astype(BF16)
        part = jnp.dot(weights, cache_v[b, :, :latent], preferred_element_type=F32)
        for g in range(groups):
            part_send[g, b] = part[g * heads : (g + 1) * heads].astype(BF16)
            log_send[g, b] = log_total[g * heads : (g + 1) * heads]

    for d in range(1, groups):
        exchange(d, log_send, log_all, log_ss, log_rs, True).start()
        exchange(d, part_send, part_all, part_ss, part_rs, True).start()
    part_all[kvp] = part_send[kvp]
    log_all[kvp] = log_send[kvp]
    load_uv().wait()
    for d in range(1, groups):
        exchange(d, log_send, log_all, log_ss, log_rs, False).wait_recv()
        exchange(d, part_send, part_all, part_ss, part_rs, False).wait_recv()

    logs = [log_all[g] for g in range(groups)]
    highest = functools.reduce(jnp.maximum, logs)
    overall = highest + jnp.log(sum(jnp.exp(x - highest) for x in logs))
    factors = [jnp.exp(x - overall) for x in logs]
    for c in range(0, latent, 128):
        olat_s[:, :, c : c + 128] = sum(
            factors[g] * part_all[g, :, :, c : c + 128].astype(F32) for g in range(groups)
        )
    for i in range(heads):
        head_s[:, i * head_dim : (i + 1) * head_dim] = jnp.dot(
            olat_s[:, i, :].astype(BF16), uv_v[i], preferred_element_type=F32
        ).astype(BF16)

    def scatter(d, source, target, ss, rs, ahead):
        other = lax.rem(me + d, count) if ahead else lax.rem(me + count - d, count)
        return pltpu.make_async_remote_copy(
            src_ref=source.at[other] if source is not ag_send else source,
            dst_ref=target.at[me if ahead else other],
            send_sem=ss.at[d],
            recv_sem=rs.at[me if ahead else other],
            device_id=peer(other),
            device_id_type=MESH,
        )

    def send_all(source, target, ss, rs):
        @pl.loop(1, count)
        def _(d):
            scatter(d, source, target, ss, rs, True).start()

    def receive_all(source, target, ss, rs):
        @pl.loop(1, count)
        def _(d):
            scatter(d, source, target, ss, rs, False).wait_recv()

    def sent_all(source, target, ss, rs):
        @pl.loop(1, count)
        def _(d):
            scatter(d, source, target, ss, rs, True).wait_send()

    @pl.loop(0, chunks)
    def _(j):
        load_wo(j).wait()
        term = jnp.dot(head_s[...], big_v[j, :out_rows], preferred_element_type=F32)
        for p in range(per_chunk):
            rs_send[j * per_chunk + p] = term[:, p * share : (p + 1) * share].astype(BF16)
        load_wd(j).start()

    send_all(rs_send, rs_all, rs_ss, rs_rs)
    rs_all[me] = rs_send[me]
    receive_all(rs_send, rs_all, rs_ss, rs_rs)
    residual = hid_s[me]
    for s in range(count):
        residual = residual + rs_all[s].astype(F32)
    hid_s[me] = residual
    ag_send[...] = residual.astype(BF16)
    send_all(ag_send, ag_all, ag_ss, ag_rs)
    ag_all[me] = ag_send[...]
    receive_all(ag_send, ag_all, ag_ss, ag_rs)

    square = jnp.zeros((batch, share), F32)
    for s in range(count):
        value = ag_all[s].astype(F32)
        square = square + value * value
        wide_s[:, s * share : (s + 1) * share] = value
    mean_square = jnp.sum(square, axis=1, keepdims=True) / width
    inverse = lax.rsqrt(mean_square + 1e-06)
    norm_s[...] = (wide_s[...] * inverse * gain_ref[...]).astype(BF16)

    def hidden_units(j, totals):
        load_wg(j).wait()
        load_wu(j).wait()
        x = norm_s[:, cols(j)]
        return (
            totals[0] + jnp.dot(x, wg_v[cols(j)], preferred_element_type=F32),
            totals[1] + jnp.dot(x, wu_v[cols(j)], preferred_element_type=F32),
        )

    zero = jnp.zeros((batch, wg_v.shape[1]), F32)
    gate, up = lax.fori_loop(0, chunks, hidden_units, (zero, zero))
    act = (gate / (1.0 + jnp.exp(-gate)) * up).astype(BF16)

    @pl.loop(0, chunks)
    def _(j):
        load_wd(j).wait()
        term = jnp.dot(act, big_v[j], preferred_element_type=F32)
        for p in range(per_chunk):
            fs_send[j * per_chunk + p] = term[:, p * share : (p + 1) * share].astype(BF16)

    send_all(fs_send, fs_all, fs_ss, fs_rs)
    fs_all[me] = fs_send[me]
    receive_all(fs_send, fs_all, fs_ss, fs_rs)
    total = hid_s[me]
    for s in range(count):
        total = total + fs_all[s].astype(F32)
    out_ref[...] = total.astype(BF16)

    for d in range(1, groups):
        exchange(d, q_send, q_all, q_ss, q_rs, True).wait_send()
        exchange(d, log_send, log_all, log_ss, log_rs, True).wait_send()
        exchange(d, part_send, part_all, part_ss, part_rs, True).wait_send()
    sent_all(rs_send, rs_all, rs_ss, rs_rs)
    sent_all(ag_send, ag_all, ag_ss, ag_rs)
    sent_all(fs_send, fs_all, fs_ss, fs_rs)


def per_device(*operands):
    (hidden_in, queries_nope, queries_rope, cache, lengths, w_uk, w_uv, w_out, norm_gain,
     w_gate, w_up, w_down) = operands
    groups, tps = lax.axis_size("kvp"), lax.axis_size("tp")
    count = groups * tps
    batch, heads, head_dim = queries_nope.shape
    latent, rope, ctx = w_uk.shape[2], queries_rope.shape[2], cache.shape[1]
    width = hidden_in.shape[1]
    share = width // count
    ff = w_gate.shape[1]
    rows = w_out.shape[0]
    per_chunk = 1
    while share * per_chunk % 128 and per_chunk < count:
        per_chunk *= 2
    chunk = share * per_chunk
    held = (w_gate.size + w_up.size + max(rows, ff) * width + cache.size + w_uk.size + w_uv.size) * 2
    fits = (
        batch % 8 == 0
        and heads % 8 == 0
        and all(size % 128 == 0 for size in (head_dim, latent, ctx, chunk, ff))
        and count % per_chunk == 0
        and rows <= ff
        and held < VMEM_BYTES - 8 * 2**20
    )
    if not fits:
        return plain_device(*operands)
    chunks = width // chunk
    dma = pltpu.SemaphoreType.DMA
    vmem = pl.BlockSpec(memory_space=pltpu.VMEM)
    anywhere = pl.BlockSpec(memory_space=pl.ANY)
    spread = pltpu.VMEM((count, batch, share), BF16)
    scratch = [
        pltpu.VMEM(cache.shape, BF16),
        pltpu.VMEM(w_uk.shape, BF16),
        pltpu.VMEM(w_uv.shape, BF16),
        pltpu.VMEM((chunks, ff, chunk), BF16),
        pltpu.VMEM(w_gate.shape, BF16),
        pltpu.VMEM(w_up.shape, BF16),
        pltpu.VMEM((batch, heads, head_dim), F32),
        pltpu.VMEM((batch, heads, latent), F32),
        pltpu.VMEM((batch, heads, latent + rope), BF16),
        pltpu.VMEM((groups, batch, heads, latent + rope), BF16),
        pltpu.VMEM((batch, groups * heads, ctx), F32),
        pltpu.VMEM((groups, batch, heads, latent), BF16),
        pltpu.VMEM((groups, batch, heads, latent), BF16),
        pltpu.VMEM((groups, batch, heads, 128), F32),
        pltpu.VMEM((groups, batch, heads, 128), F32),
        pltpu.VMEM((batch, heads, latent), F32),
        pltpu.VMEM((batch, heads * head_dim), BF16),
        pltpu.VMEM((count, batch, share), F32),
        spread,
        spread,
        pltpu.VMEM((batch, share), BF16),
        spread,
        pltpu.VMEM((batch, width), F32),
        pltpu.VMEM((batch, width), BF16),
        spread,
        spread,
        dma, dma, dma,
        dma((chunks,)), dma((chunks,)), dma((chunks,)), dma((chunks,)),
    ] + [dma((groups,))] * 6 + [dma((count,))] * 6
    return pl.pallas_call(
        functools.partial(layer_kernel, groups, tps, share, chunk, rows),
        out_shape=jax.ShapeDtypeStruct((batch, share), BF16),
        in_specs=[vmem, vmem, vmem, pl.BlockSpec(memory_space=pltpu.SMEM), vmem] + [anywhere] * 7,
        out_specs=vmem,
        scratch_shapes=scratch,
        compiler_params=pltpu.CompilerParams(
            collective_id=0, has_side_effects=True, vmem_limit_bytes=VMEM_BYTES
        ),
    )(
        hidden_in, queries_nope, queries_rope, lengths, norm_gain.reshape(1, width),
        cache, w_uk, w_uv, w_out, w_gate, w_up, w_down,
    )


def solution(mesh):
    placed = (
        P("grp", None),
        P("grp", ("kvp", "tp"), None),
        P("grp", ("kvp", "tp"), None),
        P("grp", "kvp", None),
        P("grp"),
        P(("kvp", "tp"), None, None),
        P(("kvp", "tp"), None, None),
        P(("kvp", "tp"), None),
        P(),
        P(None, ("kvp", "tp")),
        P(None, ("kvp", "tp")),
        P(("kvp", "tp"), None),
    )
    return jax.shard_map(
        per_device, mesh=mesh, in_specs=placed, out_specs=P("grp", ("kvp", "tp")), check_vma=False
    )
```

```python
import functools

import jax
import jax.numpy as jnp
from jax import lax
from jax.experimental import pallas as pl
from jax.experimental.pallas import tpu as pltpu
from jax.sharding import PartitionSpec as P


def project(o_lat, w_uv, w_out):
    head_out = jnp.einsum("bhl,hle->bhe", o_lat, w_uv, preferred_element_type=jnp.float32).astype(
        jnp.bfloat16
    )
    return jnp.dot(
        head_out.reshape(head_out.shape[0], -1), w_out, preferred_element_type=jnp.float32
    )


def plain_device(
    hidden_in,
    queries_nope,
    queries_rope,
    cache,
    lengths,
    w_uk,
    w_uv,
    w_out,
    norm_gain,
    w_gate,
    w_up,
    w_down,
):
    batch, heads_dev, head_dim = queries_nope.shape
    latent = w_uk.shape[2]
    ctx_dev = cache.shape[1]
    groups = lax.axis_size("kvp")
    score_scale = float(head_dim + queries_rope.shape[2]) ** (-0.5)
    q_lat = jnp.einsum(
        "bhd,hdl->bhl", queries_nope, w_uk, preferred_element_type=jnp.float32
    ).astype(jnp.bfloat16)
    q_lat_all, rope_all = (
        lax.all_gather(q_lat, "kvp", axis=1, tiled=True),
        lax.all_gather(queries_rope, "kvp", axis=1, tiled=True),
    )
    q_full = jnp.concatenate([q_lat_all, rope_all], axis=2)
    scores = (
        jnp.einsum("bhc,btc->bht", q_full, cache, preferred_element_type=jnp.float32) * score_scale
    )
    offset = lax.axis_index("kvp") * ctx_dev
    visible = ((offset + jnp.arange(ctx_dev, dtype=jnp.int32))[None, :] < lengths[:, None])[
        :, None, :
    ]
    masked = jnp.where(visible, scores, jnp.float32(-1e30))
    block_max = jnp.max(masked, axis=2)
    exponent = jnp.where(visible, jnp.exp(masked - block_max[..., None]), jnp.float32(0.0))
    guarded = jnp.maximum(jnp.sum(exponent, axis=2), 1.0)
    log_total = block_max + jnp.log(guarded)
    weights = (exponent / guarded[..., None]).astype(jnp.bfloat16)
    partial_value = jnp.einsum("bht,btc->bhc", weights, cache, preferred_element_type=jnp.float32)[
        ..., :latent
    ]
    blocks = partial_value.reshape(batch, groups, heads_dev, latent)
    block_logs = log_total.reshape(batch, groups, heads_dev)
    part_blocks = lax.all_to_all(
        blocks.astype(jnp.bfloat16), "kvp", split_axis=1, concat_axis=1, tiled=True
    ).astype(blocks.dtype)
    part_logs = lax.all_to_all(
        block_logs.astype(jnp.bfloat16), "kvp", split_axis=1, concat_axis=1, tiled=True
    ).astype(block_logs.dtype)
    highest = jnp.max(part_logs, axis=1)
    overall = highest + jnp.log(jnp.sum(jnp.exp(part_logs - highest[:, None, :]), axis=1))
    scaled = jnp.exp(part_logs - overall[:, None, :])[..., None] * part_blocks
    o_lat = jnp.sum(scaled, axis=1).astype(jnp.bfloat16)
    attention = project(o_lat, w_uv, w_out)
    model_width = norm_gain.shape[0]
    share_width = model_width // lax.axis_size(("kvp", "tp"))
    share_start = lax.axis_index(("kvp", "tp")) * share_width
    attn_whole = lax.psum(attention, ("kvp", "tp"))
    residual = hidden_in.astype(jnp.float32) + attn_whole
    mean_square = jnp.mean(residual * residual, axis=1)
    normed = (residual * lax.rsqrt(mean_square + 1e-06)[:, None] * norm_gain[None, :]).astype(
        jnp.bfloat16
    )
    residual_share = lax.dynamic_slice_in_dim(residual, share_start, share_width, 1)
    gate_proj = jnp.dot(normed, w_gate, preferred_element_type=jnp.float32)
    up_proj = jnp.dot(normed, w_up, preferred_element_type=jnp.float32)
    act = (jax.nn.silu(gate_proj) * up_proj).astype(jnp.bfloat16)
    ffn_terms = jnp.dot(act, w_down, preferred_element_type=jnp.float32)
    ffn_share = lax.psum_scatter(ffn_terms, ("kvp", "tp"), scatter_dimension=1, tiled=True)
    return (residual_share + ffn_share).astype(jnp.bfloat16)


MESH = pl.DeviceIdType.MESH
F32 = jnp.float32
BF16 = jnp.bfloat16
VMEM_BYTES = 67043328


def layer_kernel(
    groups, tps, share, chunk, out_rows,
    hidden_ref, nope_ref, rope_ref, len_ref, gain_ref,
    cache_hbm, uk_hbm, uv_hbm, wo_hbm, wg_hbm, wu_hbm, wd_hbm,
    out_ref,
    cache_v, uk_v, uv_v, big_v, wg_v, wu_v,
    nope_s, qlat_s, q_send, q_all, score_s, part_send, part_all, log_send, log_all,
    olat_s, head_s, hid_s, rs_send, rs_all, ag_send, ag_all, wide_s, norm_s, fs_send, fs_all,
    uk_sem, cache_sem, uv_sem, wo_sem, wg_sem, wu_sem, wd_sem,
    q_ss, q_rs, part_ss, part_rs, log_ss, log_rs, rs_ss, rs_rs, ag_ss, ag_rs, fs_ss, fs_rs,
):
    count = groups * tps
    kvp = lax.axis_index("kvp")
    tp = lax.axis_index("tp")
    me = kvp * tps + tp
    batch, heads, head_dim = nope_ref.shape
    latent = uk_v.shape[2]
    rope = rope_ref.shape[2]
    ctx = cache_v.shape[2]
    width = hidden_ref.shape[1]
    chunks = width // chunk
    per_chunk = chunk // share

    def peer(index):
        return {"kvp": index // tps, "tp": index % tps}

    def turn(step):
        return lax.rem(me // per_chunk + 1 + step, chunks)

    def load_uk():
        return pltpu.make_async_copy(uk_hbm, uk_v, uk_sem)

    def load_cache():
        return pltpu.make_async_copy(cache_hbm, cache_v, cache_sem)

    def load_uv():
        return pltpu.make_async_copy(uv_hbm, uv_v, uv_sem)

    def cols(j):
        return pl.ds(pl.multiple_of(j * chunk, 128), chunk)

    def load_wo(j):
        return pltpu.make_async_copy(
            wo_hbm.at[:, cols(j)], big_v.at[j, pl.ds(0, out_rows)], wo_sem.at[j]
        )

    def load_wd(j):
        return pltpu.make_async_copy(wd_hbm.at[:, cols(j)], big_v.at[j], wd_sem.at[j])

    def load_wg(j):
        return pltpu.make_async_copy(wg_hbm.at[cols(j)], wg_v.at[cols(j)], wg_sem.at[j])

    def load_wu(j):
        return pltpu.make_async_copy(wu_hbm.at[cols(j)], wu_v.at[cols(j)], wu_sem.at[j])

    load_uk().start()
    load_cache().start()

    barrier = pltpu.get_barrier_semaphore()

    @pl.loop(1, count)
    def _(d):
        pl.semaphore_signal(
            barrier, inc=1, device_id=peer(lax.rem(me + d, count)), device_id_type=MESH
        )

    nope_s[...] = nope_ref[...].astype(F32)
    for s in range(count):
        hid_s[s] = hidden_ref[:, s * share : (s + 1) * share].astype(F32)
    load_uk().wait()
    load_uv().start()

    @pl.loop(0, chunks)
    def _(step):
        load_wo(turn(step)).start()

    for i in range(heads):
        qlat_s[:, i, :] = jnp.dot(
            nope_s[:, i, :].astype(BF16), uk_v[i], preferred_element_type=F32
        )
    q_send[:, :, :latent] = qlat_s[...].astype(BF16)
    q_send[:, :, latent:] = rope_ref[...]
    pl.semaphore_wait(barrier, count - 1)

    def exchange(d, source, target, ss, rs, ahead):
        other = lax.rem(kvp + d, groups) if ahead else lax.rem(kvp + groups - d, groups)
        return pltpu.make_async_remote_copy(
            src_ref=source.at[other] if source is not q_send else source,
            dst_ref=target.at[kvp if ahead else other],
            send_sem=ss.at[d],
            recv_sem=rs.at[kvp if ahead else other],
            device_id={"kvp": other, "tp": tp},
            device_id_type=MESH,
        )

    for d in range(1, groups):
        exchange(d, q_send, q_all, q_ss, q_rs, True).start()

    @pl.loop(0, chunks)
    def _(j):
        load_wg(j).start()
        load_wu(j).start()

    q_all[kvp] = q_send[...]
    load_cache().wait()
    for d in range(1, groups):
        exchange(d, q_send, q_all, q_ss, q_rs, False).wait_recv()

    scale = float(head_dim + rope) ** (-0.5)
    rows = groups * heads
    for b in range(batch):
        q = q_all[:, b].astype(F32).reshape(rows, latent + rope)
        score_s[b] = (
            jnp.dot(
                q[:, :latent].astype(BF16), cache_v[b, :latent],
                preferred_element_type=F32,
            )
            + jnp.dot(
                q[:, latent:].astype(BF16), cache_v[b, latent:],
                preferred_element_type=F32,
            )
        ) * scale
    position = kvp * ctx + lax.broadcasted_iota(jnp.int32, (rows, ctx), 1)
    for b in range(batch):
        visible = position < len_ref[b]
        masked = jnp.where(visible, score_s[b], F32(-1e30))
        top = jnp.max(masked, axis=1, keepdims=True)
        exps = jnp.where(visible, jnp.exp(masked - top), F32(0.0))
        guarded = jnp.maximum(jnp.sum(exps, axis=1, keepdims=True), 1.0)
        log_total = jnp.broadcast_to(top + jnp.log(guarded), (rows, 128))
        weights = (exps / guarded).astype(BF16)
        part = lax.dot_general(
            weights, cache_v[b, :latent], (((1,), (1,)), ((), ())), preferred_element_type=F32
        )
        for g in range(groups):
            part_send[g, b] = part[g * heads : (g + 1) * heads].astype(BF16)
            log_send[g, b] = log_total[g * heads : (g + 1) * heads]

    for d in range(1, groups):
        exchange(d, log_send, log_all, log_ss, log_rs, True).start()
        exchange(d, part_send, part_all, part_ss, part_rs, True).start()
    part_all[kvp] = part_send[kvp]
    log_all[kvp] = log_send[kvp]
    load_uv().wait()
    for d in range(1, groups):
        exchange(d, log_send, log_all, log_ss, log_rs, False).wait_recv()
        exchange(d, part_send, part_all, part_ss, part_rs, False).wait_recv()

    logs = [log_all[g] for g in range(groups)]
    highest = functools.reduce(jnp.maximum, logs)
    overall = highest + jnp.log(sum(jnp.exp(x - highest) for x in logs))
    factors = [jnp.exp(x - overall) for x in logs]
    for c in range(0, latent, 128):
        olat_s[:, :, c : c + 128] = sum(
            factors[g] * part_all[g, :, :, c : c + 128].astype(F32) for g in range(groups)
        )
    for i in range(heads):
        head_s[:, i * head_dim : (i + 1) * head_dim] = jnp.dot(
            olat_s[:, i, :].astype(BF16), uv_v[i], preferred_element_type=F32
        ).astype(BF16)

    def scatter(d, source, target, ss, rs, ahead):
        other = lax.rem(me + d, count) if ahead else lax.rem(me + count - d, count)
        return pltpu.make_async_remote_copy(
            src_ref=source.at[other] if source is not ag_send else source,
            dst_ref=target.at[me if ahead else other],
            send_sem=ss.at[d],
            recv_sem=rs.at[me if ahead else other],
            device_id=peer(other),
            device_id_type=MESH,
        )

    def send_chunk(j, term, source, target, ss, rs):
        for p in range(per_chunk):
            owner = j * per_chunk + p
            source[owner] = term[:, p * share : (p + 1) * share].astype(BF16)
        for p in range(per_chunk):
            owner = j * per_chunk + p

            @pl.when(owner != me)
            def _():
                scatter(
                    lax.rem(owner - me + count, count), source, target, ss, rs, True
                ).start()

    def send_all(source, target, ss, rs):
        @pl.loop(1, count)
        def _(d):
            scatter(d, source, target, ss, rs, True).start()

    def receive_all(source, target, ss, rs):
        @pl.loop(1, count)
        def _(d):
            scatter(d, source, target, ss, rs, False).wait_recv()

    def sent_all(source, target, ss, rs):
        @pl.loop(1, count)
        def _(d):
            scatter(d, source, target, ss, rs, True).wait_send()

    @pl.loop(0, chunks)
    def _(step):
        j = turn(step)
        load_wo(j).wait()
        term = jnp.dot(head_s[...], big_v[j, :out_rows], preferred_element_type=F32)
        load_wd(j).start()
        send_chunk(j, term, rs_send, rs_all, rs_ss, rs_rs)

    rs_all[me] = rs_send[me]
    receive_all(rs_send, rs_all, rs_ss, rs_rs)
    residual = hid_s[me]
    for s in range(count):
        residual = residual + rs_all[s].astype(F32)
    hid_s[me] = residual
    ag_send[...] = residual.astype(BF16)
    send_all(ag_send, ag_all, ag_ss, ag_rs)
    ag_all[me] = ag_send[...]
    receive_all(ag_send, ag_all, ag_ss, ag_rs)

    square = jnp.zeros((batch, share), F32)
    for s in range(count):
        value = ag_all[s].astype(F32)
        square = square + value * value
        wide_s[:, s * share : (s + 1) * share] = value
    mean_square = jnp.sum(square, axis=1, keepdims=True) / width
    inverse = lax.rsqrt(mean_square + 1e-06)
    norm_s[...] = (wide_s[...] * inverse * gain_ref[...]).astype(BF16)

    def hidden_units(j, totals):
        load_wg(j).wait()
        load_wu(j).wait()
        x = norm_s[:, cols(j)]
        return (
            totals[0] + jnp.dot(x, wg_v[cols(j)], preferred_element_type=F32),
            totals[1] + jnp.dot(x, wu_v[cols(j)], preferred_element_type=F32),
        )

    zero = jnp.zeros((batch, wg_v.shape[1]), F32)
    gate, up = lax.fori_loop(0, chunks, hidden_units, (zero, zero))
    act = (gate / (1.0 + jnp.exp(-gate)) * up).astype(BF16)

    @pl.loop(0, chunks)
    def _(step):
        j = turn(step)
        load_wd(j).wait()
        term = jnp.dot(act, big_v[j], preferred_element_type=F32)
        send_chunk(j, term, fs_send, fs_all, fs_ss, fs_rs)

    fs_all[me] = fs_send[me]
    receive_all(fs_send, fs_all, fs_ss, fs_rs)
    total = hid_s[me]
    for s in range(count):
        total = total + fs_all[s].astype(F32)
    out_ref[...] = total.astype(BF16)

    for d in range(1, groups):
        exchange(d, q_send, q_all, q_ss, q_rs, True).wait_send()
        exchange(d, log_send, log_all, log_ss, log_rs, True).wait_send()
        exchange(d, part_send, part_all, part_ss, part_rs, True).wait_send()
    sent_all(rs_send, rs_all, rs_ss, rs_rs)
    sent_all(ag_send, ag_all, ag_ss, ag_rs)
    sent_all(fs_send, fs_all, fs_ss, fs_rs)


def per_device(*operands):
    (hidden_in, queries_nope, queries_rope, cache, lengths, w_uk, w_uv, w_out, norm_gain,
     w_gate, w_up, w_down) = operands
    groups, tps = lax.axis_size("kvp"), lax.axis_size("tp")
    count = groups * tps
    batch, heads, head_dim = queries_nope.shape
    latent, rope, ctx = w_uk.shape[2], queries_rope.shape[2], cache.shape[1]
    width = hidden_in.shape[1]
    share = width // count
    ff = w_gate.shape[1]
    rows = w_out.shape[0]
    per_chunk = 1
    while share * per_chunk % 128 and per_chunk < count:
        per_chunk *= 2
    chunk = share * per_chunk
    held = (w_gate.size + w_up.size + max(rows, ff) * width + cache.size + w_uk.size + w_uv.size) * 2
    fits = (
        batch % 8 == 0
        and heads % 8 == 0
        and all(size % 128 == 0 for size in (head_dim, latent, ctx, chunk, ff))
        and count % per_chunk == 0
        and rows <= ff
        and held < VMEM_BYTES - 8 * 2**20
    )
    if not fits:
        return plain_device(*operands)
    chunks = width // chunk
    dma = pltpu.SemaphoreType.DMA
    vmem = pl.BlockSpec(memory_space=pltpu.VMEM)
    anywhere = pl.BlockSpec(memory_space=pl.ANY)
    spread = pltpu.VMEM((count, batch, share), BF16)
    scratch = [
        pltpu.VMEM((batch, latent + rope, ctx), BF16),
        pltpu.VMEM(w_uk.shape, BF16),
        pltpu.VMEM(w_uv.shape, BF16),
        pltpu.VMEM((chunks, ff, chunk), BF16),
        pltpu.VMEM(w_gate.shape, BF16),
        pltpu.VMEM(w_up.shape, BF16),
        pltpu.VMEM((batch, heads, head_dim), F32),
        pltpu.VMEM((batch, heads, latent), F32),
        pltpu.VMEM((batch, heads, latent + rope), BF16),
        pltpu.VMEM((groups, batch, heads, latent + rope), BF16),
        pltpu.VMEM((batch, groups * heads, ctx), F32),
        pltpu.VMEM((groups, batch, heads, latent), BF16),
        pltpu.VMEM((groups, batch, heads, latent), BF16),
        pltpu.VMEM((groups, batch, heads, 128), F32),
        pltpu.VMEM((groups, batch, heads, 128), F32),
        pltpu.VMEM((batch, heads, latent), F32),
        pltpu.VMEM((batch, heads * head_dim), BF16),
        pltpu.VMEM((count, batch, share), F32),
        spread,
        spread,
        pltpu.VMEM((batch, share), BF16),
        spread,
        pltpu.VMEM((batch, width), F32),
        pltpu.VMEM((batch, width), BF16),
        spread,
        spread,
        dma, dma, dma,
        dma((chunks,)), dma((chunks,)), dma((chunks,)), dma((chunks,)),
    ] + [dma((groups,))] * 6 + [dma((count,))] * 6
    return pl.pallas_call(
        functools.partial(layer_kernel, groups, tps, share, chunk, rows),
        out_shape=jax.ShapeDtypeStruct((batch, share), BF16),
        in_specs=[vmem, vmem, vmem, pl.BlockSpec(memory_space=pltpu.SMEM), vmem] + [anywhere] * 7,
        out_specs=vmem,
        scratch_shapes=scratch,
        compiler_params=pltpu.CompilerParams(
            collective_id=0, has_side_effects=True, vmem_limit_bytes=VMEM_BYTES
        ),
    )(
        hidden_in, queries_nope, queries_rope, lengths, norm_gain.reshape(1, width),
        jnp.swapaxes(cache, 1, 2), w_uk, w_uv, w_out, w_gate, w_up, w_down,
    )


def solution(mesh):
    placed = (
        P("grp", None),
        P("grp", ("kvp", "tp"), None),
        P("grp", ("kvp", "tp"), None),
        P("grp", "kvp", None),
        P("grp"),
        P(("kvp", "tp"), None, None),
        P(("kvp", "tp"), None, None),
        P(("kvp", "tp"), None),
        P(),
        P(None, ("kvp", "tp")),
        P(None, ("kvp", "tp")),
        P(("kvp", "tp"), None),
    )
    return jax.shard_map(
        per_device, mesh=mesh, in_specs=placed, out_specs=P("grp", ("kvp", "tp")), check_vma=False
    )
```
